32 devices in a mesh: section: 8 (over z, core), ep: 4 (over y, x).
Axes of the slice: x: 2, y: 2, z: 4, core: 2. Of those that a mesh axis runs over, the one named last changes fastest.
Arguments:
- states: bfloat16 [512, 3072], P(('section', 'ep')), may hold values from -6 to 6
- entering: bfloat16 [64, 3072], P('ep'), may hold values from -6 to 6
- seq_lens: int32 [9, 64], replicated, may hold values from 1 to 16, 512 in all within a row
- routes: int32 [8, 2, 64, 2], P('section', None, 'ep'), may hold values from 0 to 7, all different within a row; in each aligned block of 16 rows (0 to 15, 16 to 31, ..., all dimensions but the last counted through in order) at most 8 rows name the same one
- attn_norm: bfloat16 [8, 3072], P('section'), may hold values from 0.099609375 to 1.8984375
- ffn_norm: bfloat16 [8, 3072], P('section'), may hold values from 0.099609375 to 1.8984375
- wq: bfloat16 [8, 3072, 4096], P('section', None, 'ep'), may hold values from -0.109375 to 0.109375
- wk: bfloat16 [8, 3072, 1024], P('section', None, 'ep'), may hold values from -0.109375 to 0.109375
- wv: bfloat16 [8, 3072, 1024], P('section', None, 'ep'), may hold values from -0.109375 to 0.109375
- wo: bfloat16 [8, 4096, 3072], P('section', 'ep'), may hold values from -0.09375 to 0.09375
- router: bfloat16 [8, 3072, 8], P('section'), may hold values from -0.21875 to 0.21875
- w_gate: bfloat16 [8, 3072, 7168], P('section', None, 'ep'), may hold values from -0.109375 to 0.109375
- w_up: bfloat16 [8, 3072, 7168], P('section', None, 'ep'), may hold values from -0.109375 to 0.109375
- w_down: bfloat16 [8, 7168, 3072], P('section', 'ep'), may hold values from -0.125 to 0.125
- cache_k: bfloat16 [8, 2, 64, 8, 16, 128], P('section', None, 'ep'), may hold values from -127 to 127, as said below
- cache_v: bfloat16 [8, 2, 64, 8, 16, 128], P('section', None, 'ep'), may hold values from -127 to 127, as said below
- k_scale: float32 [8, 2, 64, 8, 4], P('section', None, 'ep'), may hold values from 0.004 to 2.4
- v_scale: float32 [8, 2, 64, 8, 4], P('section', None, 'ep'), may hold values from 0.004 to 0.04
Outputs:
- advanced: bfloat16 [512, 3072], P(('section', 'ep'))
The draws below stay inside these ranges and needn't reach their ends.
Inputs may be any that keep to these rules, and one draw needn't show every extreme that they name: `seq_lens`: each row holds 64 lengths; the longest is exactly 16. `routes`: the two ids of a token differ. In the rows of one device (aligned blocks of 16 tokens of a section and step) no expert is named by more than 8 tokens. `cache_k`: whole numbers. `cache_v`: whole numbers.
All inputs are finite; a program needn't handle non-finite values.
Results may differ from the reference program's by a relative error of at most 0.033.
Values may be sent and summed in bfloat16 or wider, within the bound.
A program may use at most 128 MiB of HBM per device.

```python
import math
import jax
import jax.numpy as jnp
import numpy as np
from jax import lax

D = 3072
QH = 32
KVH = 8
HD = 128
EXPERTS = 8
EXP_WIN = 1
FFE = 7168
TOK_DEV = 16
LEN = 16
BLK = 4
TICKS = 2
SECTIONS = 8
MICRO = 9
MBS = 64
NBLK = 4
CAP = 8


def draw_cache_k(key, part):
    codes = jax.random.randint(jax.random.fold_in(key, 11), (SECTIONS, TICKS, MBS, KVH, LEN, HD), -127, 128)
    return codes.astype(jnp.float32).astype(jnp.bfloat16)


def draw_cache_v(key, part):
    codes = jax.random.randint(jax.random.fold_in(key, 12), (SECTIONS, TICKS, MBS, KVH, LEN, HD), -127, 128)
    return codes.astype(jnp.float32).astype(jnp.bfloat16)


def draw_k_scale(key, part):
    shape = (SECTIONS, TICKS, MBS, KVH, NBLK)
    base = jnp.exp(jax.random.uniform(jax.random.fold_in(key, 21), shape, jnp.float32, jnp.log(0.004), jnp.log(0.04)))
    return base


def draw_v_scale(key, part):
    shape = (SECTIONS, TICKS, MBS, KVH, NBLK)
    return jnp.exp(jax.random.uniform(jax.random.fold_in(key, 32), shape, jnp.float32, jnp.log(0.004), jnp.log(0.04)))


def steps_of(rng, dims, cuts, low, largest):
    def one(dim, blocks):
        steps = jax.random.uniform(jax.random.fold_in(jax.random.fold_in(rng, 6), dim), (blocks,), jnp.float32, low / len(cuts), largest / len(cuts))
        return jnp.repeat(jnp.exp(steps), dims[dim] // blocks).reshape((-1,) + (1,) * (len(dims) - dim - 1))

    gain = one(*cuts[0])
    for cut in cuts[1:]:
        gain = gain * one(*cut)
    return gain


def length_profile(number_of, total, limit, slope):
    weights = [(1 << 20) // math.isqrt(rank ** slope) + 1 for rank in range(2, number_of + 1)]
    rest, given = total - limit - (number_of - 1), [1] * (number_of - 1)
    while rest > 0:
        movable = [i for i in range(number_of - 1) if given[i] < limit]
        whole, remaining = sum([weights[i] for i in movable]), rest
        for i in movable:
            extra = min(limit - given[i], max(1, remaining * weights[i] // whole), rest)
            given[i] = given[i] + extra
            rest = rest - extra
    return np.array([limit] + given)


def uneven(key, amount, total, limit, slope):
    if amount == 2:
        one = jax.random.randint(key, (), max(1, total - limit), min(limit, total - 1) + 1)
        return jnp.stack([one, total - one])
    tallies = jnp.asarray(length_profile(amount, total, limit, slope), jnp.int32)
    couples = (amount - 1) // 2
    donor, sink = tallies[1:1 + 2 * couples:2], tallies[2:2 + 2 * couples:2]
    margin = jnp.minimum(donor - 1, limit - sink)
    passed = jax.random.randint(jax.random.fold_in(key, 1), (couples,), 0, 1 << 20) % (margin + 1)
    tallies = tallies.at[1:1 + 2 * couples:2].set(donor - passed).at[2:2 + 2 * couples:2].set(sink + passed)
    return tallies[jax.random.permutation(jax.random.fold_in(key, 2), amount)]


def deal_out(key, own, number, rows, number_of, top, bound, skew):
    ranking = jax.random.permutation(key, number_of)
    crowded, ordinary = load_shares(number_of, rows * top, bound, skew, True), load_shares(number_of, rows * top, bound, skew, False)
    places = jnp.arange(number_of)

    def named(sizes, turn):
        used = int((sizes > 0).sum())
        fixed = max(1, used // 4)
        shifted = fixed + (places - fixed + turn * (used - fixed)) % max(1, number_of - fixed)
        return jnp.zeros((number_of,), jnp.int32).at[ranking[jnp.where(places < fixed, places, shifted)]].set(jnp.asarray(sizes, jnp.int32))

    sizes = jnp.where(number % 4 == 0, named(crowded, number // 4), named(ordinary, number - number // 4 - 1))
    mixed = jax.random.permutation(jax.random.fold_in(own, 3), number_of)
    giver, taker = mixed[0:number_of // 2 * 2:2], mixed[1:number_of // 2 * 2:2]
    margin = jnp.minimum(sizes[giver] - 1, bound - sizes[taker]) // 2
    margin = jnp.where((giver == ranking[0]) | (taker == ranking[0]) | (sizes[taker] == 0), 0, jnp.maximum(margin, 0))
    shifted = jax.random.randint(jax.random.fold_in(own, 4), (number_of // 2,), 0, 1 << 20) % (margin + 1)
    sizes = sizes.at[giver].add(-shifted).at[taker].add(shifted)
    items = jnp.searchsorted(jnp.cumsum(sizes), jnp.arange(rows * top), side="right").astype(jnp.int32)
    grid = items.reshape(top, rows).T
    grid = grid[jax.random.permutation(jax.random.fold_in(own, 1), rows)]
    turn = jax.random.randint(jax.random.fold_in(own, 2), (rows, 1), 0, top)
    return jnp.take_along_axis(grid, (jnp.arange(top)[None, :] + turn) % top, axis=1)


def load_shares(number_of, total, bound, skew, full):
    loads = [(1 << 20) // math.isqrt(grade ** skew) + 1 for grade in range(1, number_of + 1)]
    largest = bound if full else min(bound, max(-(-total // number_of), total * loads[0] // sum(loads)))
    least = 1 if total - largest >= number_of - 1 else 0
    holding, spare = [largest] + [least] * (number_of - 1), total - largest - least * (number_of - 1)
    while spare > 0:
        free = [i for i in range(1, number_of) if holding[i] < largest] or [i for i in range(1, number_of) if holding[i] < bound]
        whole, budget = sum([loads[i] for i in free]), spare
        for i in free:
            more = min(bound - holding[i], max(1, budget * loads[i] // whole), spare)
            holding[i] = holding[i] + more
            spare = spare - more
    return np.array(holding)


def scatter_about(key, extent, scale, limit, cuts=(), kind=jnp.bfloat16):
    array = scale * jax.random.normal(key, extent, jnp.float32)
    if cuts:
        array = array * steps_of(key, extent, cuts, -0.22, 0.18)
    return jnp.clip(array, -limit, limit).astype(kind)


def setup_inputs(seed: int = 0) -> dict:
    seeds = jax.random.split(jax.random.key(seed), 19)
    states = scatter_about(seeds[0], (SECTIONS * MBS, D), 1.0, 6.0, ((0, 32),))
    entering = scatter_about(seeds[1], (MBS, D), 1.0, 6.0, ((0, 4),))
    seq_lens = jax.vmap(lambda own: uneven(own, MBS, MBS * LEN // 2, LEN, 2))(jax.random.split(seeds[2], MICRO)).reshape((MICRO, MBS)).astype(jnp.int32)
    routes_keys = jax.random.split(jax.random.fold_in(seeds[3], 1), SECTIONS * TICKS * MBS // TOK_DEV)
    routes_turns = jax.random.permutation(jax.random.fold_in(seeds[3], 3), SECTIONS * TICKS * MBS // TOK_DEV)
    routes = jax.vmap(lambda own, number: deal_out(jax.random.fold_in(seeds[3], 2), own, number, TOK_DEV, EXPERTS, 2, CAP, 0))(routes_keys, routes_turns).reshape((SECTIONS, TICKS, MBS, 2))
    attn_norm = jnp.clip(1.0 + 0.18 * jax.random.normal(seeds[4], (SECTIONS, D), jnp.float32), 0.099609375, 1.8984375).astype(jnp.bfloat16)
    ffn_norm = jnp.clip(1.0 + 0.18 * jax.random.normal(seeds[5], (SECTIONS, D), jnp.float32), 0.099609375, 1.8984375).astype(jnp.bfloat16)
    wq = scatter_about(seeds[6], (SECTIONS, D, QH * HD), D ** -0.5, 0.109375, ((0, 8), (2, 4)))
    wk = scatter_about(seeds[7], (SECTIONS, D, KVH * HD), D ** -0.5, 0.109375, ((0, 8), (2, 4)))
    wv = scatter_about(seeds[8], (SECTIONS, D, KVH * HD), D ** -0.5, 0.109375, ((0, 8), (2, 4)))
    wo = scatter_about(seeds[9], (SECTIONS, QH * HD, D), (QH * HD) ** -0.5, 0.09375, ((0, 8), (1, 4)))
    router = scatter_about(seeds[10], (SECTIONS, D, EXPERTS), (D // 4) ** -0.5, 0.21875, ((0, 8),))
    w_gate = scatter_about(seeds[11], (SECTIONS, D, EXP_WIN * FFE), D ** -0.5, 0.109375, ((0, 8), (2, 4)))
    w_up = scatter_about(seeds[12], (SECTIONS, D, EXP_WIN * FFE), D ** -0.5, 0.109375, ((0, 8), (2, 4)))
    w_down = scatter_about(seeds[13], (SECTIONS, EXP_WIN * FFE, D), (FFE // 4) ** -0.5, 0.125, ((0, 8), (1, 4)))
    cache_k = draw_cache_k(jax.random.fold_in(seeds[18], 71), 0)
    cache_v = draw_cache_v(jax.random.fold_in(seeds[18], 71), 0)
    k_scale = draw_k_scale(jax.random.fold_in(seeds[18], 71), 0)
    v_scale = draw_v_scale(jax.random.fold_in(seeds[18], 71), 0)
    return {"states": states, "entering": entering, "seq_lens": seq_lens, "routes": routes, "attn_norm": attn_norm, "ffn_norm": ffn_norm, "wq": wq, "wk": wk, "wv": wv, "wo": wo, "router": router, "w_gate": w_gate, "w_up": w_up, "w_down": w_down, "cache_k": cache_k, "cache_v": cache_v, "k_scale": k_scale, "v_scale": v_scale}


rope_base = 1000000.0
norm_eps = 1e-05

def rms_scale(values, gain_vec):
    wide = values.astype(jnp.float32)
    factor = lax.rsqrt(lax.optimization_barrier(jnp.mean(wide * wide, axis=-1, keepdims=True)) + norm_eps)
    return (wide * factor * gain_vec.astype(jnp.float32)).astype(jnp.bfloat16)

def rotate(head_vals, lengths_now):
    half_dim = head_vals.shape[-1] // 2
    inv_freq = rope_base ** (-jnp.arange(half_dim, dtype=jnp.float32) * 2.0 / head_vals.shape[-1])
    angles = lengths_now.astype(jnp.float32)[:, None, None] * inv_freq[None, None, :]
    cosine_vals = jnp.cos(angles)
    sine_table = jnp.sin(angles)
    wide = head_vals.astype(jnp.float32)
    lower_half = wide[..., :half_dim]
    upper_half = wide[..., half_dim:]
    turned = jnp.concatenate([lower_half * cosine_vals - upper_half * sine_table, upper_half * cosine_vals + lower_half * sine_table], axis=-1)
    return turned.astype(jnp.bfloat16)

def layer(layer_in, lengths_now, chosen, attn_gain, ffn_gain, wq, wk, wv, wo, router, w_gate, w_up, w_down, key_codes, value_codes, key_scale, value_scale):
    row_count = layer_in.shape[0]
    group_size = QH // KVH
    inverse_square_root = HD ** (-0.5)
    normed = rms_scale(layer_in, attn_gain)
    query_rows = jnp.dot(normed, wq, preferred_element_type=jnp.float32).astype(jnp.bfloat16)
    fresh_key_rows = jnp.dot(normed, wk, preferred_element_type=jnp.float32).astype(jnp.bfloat16)
    value_new = jnp.dot(normed, wv, preferred_element_type=jnp.float32).astype(jnp.bfloat16)
    query_rows = rotate(query_rows.reshape(row_count, QH, HD), lengths_now).reshape(row_count, KVH, group_size, HD)
    fresh_key_rows = rotate(fresh_key_rows.reshape(row_count, KVH, HD), lengths_now)
    value_new = value_new.reshape(row_count, KVH, HD)
    raw_scores = jnp.einsum('bkgd,bkpd->bkgp', query_rows.astype(jnp.float32), key_codes.astype(jnp.float32))
    key_scales = jnp.repeat(key_scale, BLK, axis=-1)
    value_scales = jnp.repeat(value_scale, BLK, axis=-1)
    scores = raw_scores * key_scales[:, :, None, :] * inverse_square_root
    visible = (jnp.arange(LEN, dtype=jnp.int32)[None, :] < lengths_now[:, None])[:, None, None, :]
    current_token_score = jnp.einsum('rwqs,rws->rwq', query_rows.astype(jnp.float32), fresh_key_rows.astype(jnp.float32)) * inverse_square_root
    row_top = jnp.maximum(lax.optimization_barrier(jnp.max(jnp.where(visible, scores, -1e+30), axis=-1)), current_token_score)
    exponent = jnp.where(visible, jnp.exp(scores - row_top[..., None]), 0.0)
    self_weight = jnp.exp(current_token_score - row_top)
    denom_sum = lax.optimization_barrier(jnp.sum(exponent, axis=-1)) + self_weight
    weights = (exponent * value_scales[:, :, None, :]).astype(jnp.bfloat16)
    mixture = jnp.einsum('bkgp,bkpd->bkgd', weights.astype(jnp.float32), value_codes.astype(jnp.float32))
    mixture = mixture + self_weight[..., None] * value_new.astype(jnp.float32)[:, :, None, :]
    attended = (mixture / denom_sum[..., None]).astype(jnp.bfloat16).reshape(row_count, QH * HD)
    residual = (layer_in.astype(jnp.float32) + jnp.dot(attended, wo, preferred_element_type=jnp.float32)).astype(jnp.bfloat16)
    ffn_input = rms_scale(residual, ffn_gain)
    logits = jnp.dot(ffn_input, router, preferred_element_type=jnp.float32)
    picked = jnp.take_along_axis(logits, chosen, axis=1)
    gate_probs = jax.nn.softmax(picked, axis=-1)
    expert_sum = jnp.zeros((row_count, D), jnp.float32)
    for expert_id in range(EXP_WIN):
        gate_act = jnp.dot(ffn_input, w_gate[:, expert_id * FFE:(expert_id + 1) * FFE], preferred_element_type=jnp.float32)
        up_act = jnp.dot(ffn_input, w_up[:, expert_id * FFE:(expert_id + 1) * FFE], preferred_element_type=jnp.float32)
        hidden = (jax.nn.silu(gate_act) * up_act).astype(jnp.bfloat16)
        expert_out = jnp.dot(hidden, w_down[expert_id * FFE:(expert_id + 1) * FFE], preferred_element_type=jnp.float32)
        share = lax.optimization_barrier(jnp.sum(jnp.where(chosen == expert_id, gate_probs, 0.0), axis=-1))
        expert_sum = expert_sum + share[:, None] * expert_out
    return (residual.astype(jnp.float32) + expert_sum).astype(jnp.bfloat16)

def reference(states, entering, seq_lens, routes, attn_norm, ffn_norm, wq, wk, wv, wo, router, w_gate, w_up, w_down, cache_k, cache_v, k_scale, v_scale):

    def run_layer(section_id, tick_index, layer_in):
        return layer(layer_in, seq_lens[section_id + 1 - tick_index], routes[section_id, tick_index], attn_norm[section_id], ffn_norm[section_id], wq[section_id], wk[section_id], wv[section_id], wo[section_id], router[section_id], w_gate[section_id], w_up[section_id], w_down[section_id], cache_k[section_id, tick_index], cache_v[section_id, tick_index], k_scale[section_id, tick_index], v_scale[section_id, tick_index])
    first_tick = [run_layer(section_id, 0, states[section_id * MBS:(section_id + 1) * MBS]) for section_id in range(SECTIONS - 1)]
    second_tick = [run_layer(0, 1, entering)]
    for section_id in range(1, SECTIONS):
        second_tick.append(run_layer(section_id, 1, first_tick[section_id - 1]))
    return jnp.concatenate(second_tick, axis=0)
```

```python
import functools

import jax
import jax.numpy as jnp
from jax import lax
from jax.experimental import pallas as pl
from jax.experimental.pallas import tpu as pltpu
from jax.sharding import PartitionSpec as P

QH = 32
KVH = 8
HD = 128
EXPERTS = 8
LEN = 16
BLK = 4
GROUP = QH // KVH
TICKS = 2
PHASES = 6

rope_base = 1000000.0
norm_eps = 1e-05
F32 = jnp.float32
BF16 = jnp.bfloat16
MESH = pl.DeviceIdType.MESH


def rms_scale(values, gain_vec):
    wide = values.astype(F32)
    factor = lax.rsqrt(jnp.mean(wide * wide, axis=-1, keepdims=True) + norm_eps)
    return (wide * factor * gain_vec.astype(F32)).astype(BF16)


def tile_of(columns):
    for tile in (256, 128):
        if columns % tile == 0:
            return tile
    return columns


def over_columns(columns, body):
    tile = tile_of(columns)
    count = columns // tile
    if count == 1:
        body(slice(0, columns), tile)
        return

    @pl.loop(0, count)
    def _(i):
        body(pl.ds(pl.multiple_of(i * tile, tile), tile), tile)


def kernel(
    ep,
    sections,
    states,
    entering,
    attn_gain,
    ffn_gain,
    router,
    cache_k,
    cache_v,
    cos_t,
    sin_t,
    ks_t,
    vs_t,
    bias_t,
    hits_t,
    wq_h,
    wk_h,
    wv_h,
    wo_h,
    wg_h,
    wu_h,
    wd_h,
    out,
    wq,
    wk,
    wv,
    wo,
    wg,
    wu,
    wd,
    x_in,
    y_send,
    shift_recv,
    n_all,
    qkv_send,
    qkv_all,
    att_send,
    att_all,
    wo_send,
    wo_all,
    f_all,
    hidden,
    d_send,
    d_all,
    wsem,
    send_sem,
    recv_sem,
    shift_sem,
):
    me = lax.axis_index("ep")
    sec = lax.axis_index("section")
    rows, width = states.shape
    total = ep * rows
    q_cols = wq.shape[1]
    kv_cols = wk.shape[1]
    heads_here = q_cols // HD
    inv_root = HD ** (-0.5)

    loads = [
        pltpu.make_async_copy(src.at[0], dst, wsem.at[i])
        for i, (src, dst) in enumerate(
            [(wq_h, wq), (wk_h, wk), (wv_h, wv), (wo_h, wo), (wg_h, wg), (wu_h, wu), (wd_h, wd)]
        )
    ]
    for load in loads:
        load.start()

    barrier = pltpu.get_barrier_semaphore()
    for off in range(1, ep):
        pl.semaphore_signal(
            barrier, inc=1, device_id={"ep": lax.rem(me + off, ep)}, device_id_type=MESH
        )
    for off in (1, sections - 1):
        pl.semaphore_signal(
            barrier, inc=1, device_id={"section": lax.rem(sec + off, sections)}, device_id_type=MESH
        )
    x_in[0] = states[...]
    n_all[0, me] = rms_scale(states[...], attn_gain[...])
    pl.semaphore_wait(barrier, ep + 1)

    def exchange(tick, phase, source, target):
        copies = []
        for off in range(1, ep):
            peer = lax.rem(me + off, ep)
            copies.append(
                pltpu.make_async_remote_copy(
                    src_ref=source(peer),
                    dst_ref=target.at[tick, me],
                    send_sem=send_sem.at[tick * PHASES + phase, off - 1],
                    recv_sem=recv_sem.at[tick * PHASES + phase, off - 1],
                    device_id={"ep": peer},
                    device_id_type=MESH,
                )
            )
        for copy in copies:
            copy.start()
        return copies

    def finish(copies):
        for copy in copies:
            copy.wait()

    def split(values):
        return values.reshape(ep, rows, values.shape[-1])

    for tick in range(TICKS):
        x = x_in[tick]
        if tick:
            n_all[tick, me] = rms_scale(x, attn_gain[...])
        finish(exchange(tick, 0, lambda peer: n_all.at[tick, me], n_all))

        def project(weight, base):
            def body(cols, tile):
                got = jnp.dot(
                    n_all[tick].reshape(total, width), weight[:, cols], preferred_element_type=F32
                )
                if isinstance(cols, slice):
                    place = slice(base, base + tile)
                else:
                    place = pl.ds(pl.multiple_of(cols.start + base, tile), tile)
                qkv_send[tick, :, :, place] = split(got.astype(BF16))

            over_columns(weight.shape[1], body)

        for i, (weight, base) in enumerate(((wq, 0), (wk, q_cols), (wv, q_cols + kv_cols))):
            if tick == 0:
                loads[i].wait()
            project(weight, base)
        copies = exchange(tick, 1, lambda peer: qkv_send.at[tick, peer], qkv_all)
        qkv_all[tick, me] = qkv_send[tick, me]
        finish(copies)

        cos_v, sin_v = cos_t[tick], sin_t[tick]

        def turn(head):
            return (head * cos_v + pltpu.roll(head, HD // 2, 1) * sin_v).astype(BF16)

        def q_head(h):
            at = (h % heads_here) * HD
            return qkv_all[tick, h // heads_here, :, at : at + HD].astype(F32)

        def kv_head(base, k):
            if kv_cols >= HD:
                per = kv_cols // HD
                at = base + (k % per) * HD
                return qkv_all[tick, k // per, :, at : at + HD].astype(F32)
            per = HD // kv_cols
            return jnp.concatenate(
                [
                    qkv_all[tick, k * per + i, :, base : base + kv_cols].astype(F32)
                    for i in range(per)
                ],
                axis=-1,
            )

        for k in range(KVH):
            queries = jnp.concatenate([turn(q_head(k * GROUP + g)) for g in range(GROUP)], axis=0)
            key_new = turn(kv_head(q_cols, k)).astype(F32)
            value_new = kv_head(q_cols + kv_cols, k)
            key_codes = cache_k[0, tick, :, k].reshape(rows * LEN, HD)
            value_codes = cache_v[0, tick, :, k].reshape(rows * LEN, HD)
            raw = lax.dot_general(
                queries, key_codes, (((1,), (1,)), ((), ())), preferred_element_type=F32
            )
            scores = raw * ks_t[tick, k : k + 1] * inv_root + bias_t[tick]
            own = (
                jnp.sum(
                    queries.astype(F32) * jnp.concatenate([key_new] * GROUP, axis=0),
                    axis=-1,
                    keepdims=True,
                )
                * inv_root
            )
            top = jnp.maximum(jnp.max(scores, axis=-1, keepdims=True), own)
            exponent = jnp.exp(scores - top)
            self_weight = jnp.exp(own - top)
            denom = jnp.sum(exponent, axis=-1, keepdims=True) + self_weight
            weights = (exponent * vs_t[tick, k : k + 1]).astype(BF16)
            mixture = jnp.dot(weights, value_codes, preferred_element_type=F32)
            mixture = mixture + self_weight * jnp.concatenate([value_new] * GROUP, axis=0)
            attended = (mixture / denom).astype(BF16)
            for g in range(GROUP):
                h = k * GROUP + g
                at = (h % heads_here) * HD
                att_send[tick, h // heads_here, :, at : at + HD] = attended[
                    g * rows : (g + 1) * rows
                ]
        copies = exchange(tick, 2, lambda peer: att_send.at[tick, peer], att_all)
        att_all[tick, me] = att_send[tick, me]
        finish(copies)

        if tick == 0:
            loads[3].wait()

        def out_body(cols, tile):
            got = jnp.dot(
                att_all[tick].reshape(total, q_cols), wo[:, cols], preferred_element_type=F32
            )
            wo_send[tick, :, :, cols] = split(got.astype(BF16))

        over_columns(width, out_body)
        copies = exchange(tick, 3, lambda peer: wo_send.at[tick, peer], wo_all)
        wo_all[tick, me] = wo_send[tick, me]
        finish(copies)
        head_total = jnp.sum(wo_all[tick].astype(F32), axis=0)
        residual = (x_in[tick].astype(F32) + head_total).astype(BF16)
        ffn_input = rms_scale(residual, ffn_gain[...])
        f_all[tick, me] = ffn_input
        copies = exchange(tick, 4, lambda peer: f_all.at[tick, me], f_all)
        logits = jnp.dot(ffn_input, router[0], preferred_element_type=F32)
        first, second = hits_t[tick, 0], hits_t[tick, 1]
        pick_a = jnp.sum(logits * first, axis=-1, keepdims=True)
        pick_b = jnp.sum(logits * second, axis=-1, keepdims=True)
        best = jnp.maximum(pick_a, pick_b)
        exp_a, exp_b = jnp.exp(pick_a - best), jnp.exp(pick_b - best)
        share = (exp_a * first[:, :1] + exp_b * second[:, :1]) / (exp_a + exp_b)
        finish(copies)

        if tick == 0:
            loads[4].wait()
            loads[5].wait()

        def up_body(cols, tile):
            landed = f_all[tick].reshape(total, width)
            gate = jnp.dot(landed, wg[:, cols], preferred_element_type=F32)
            up = jnp.dot(landed, wu[:, cols], preferred_element_type=F32)
            hidden[:, cols] = (gate / (1.0 + jnp.exp(-gate)) * up).astype(BF16)

        over_columns(wg.shape[1], up_body)
        if tick == 0:
            loads[6].wait()

        def down_body(cols, tile):
            got = jnp.dot(hidden[...], wd[:, cols], preferred_element_type=F32)
            d_send[tick, :, :, cols] = split(got.astype(BF16))

        over_columns(width, down_body)
        copies = exchange(tick, 5, lambda peer: d_send.at[tick, peer], d_all)
        d_all[tick, me] = d_send[tick, me]
        finish(copies)
        expert_sum = jnp.sum(d_all[tick].astype(F32), axis=0) * share
        result = (residual.astype(F32) + expert_sum).astype(BF16)
        if tick == TICKS - 1:
            out[...] = result
        else:
            y_send[...] = result
            shift = pltpu.make_async_remote_copy(
                src_ref=y_send,
                dst_ref=shift_recv,
                send_sem=shift_sem.at[0],
                recv_sem=shift_sem.at[1],
                device_id={"section": lax.rem(sec + 1, sections)},
                device_id_type=MESH,
            )

            @pl.when(sec < sections - 1)
            def _():
                shift.start()

            @pl.when(sec == 0)
            def _():
                x_in[1] = entering[...]

            @pl.when(sec > 0)
            def _():
                shift.wait_recv()
                x_in[1] = shift_recv[...]

            @pl.when(sec < sections - 1)
            def _():
                shift.wait_send()


def local(
    states,
    entering,
    seq_lens,
    routes,
    attn_norm,
    ffn_norm,
    wq,
    wk,
    wv,
    wo,
    router,
    w_gate,
    w_up,
    w_down,
    cache_k,
    cache_v,
    k_scale,
    v_scale,
):
    ep = lax.axis_size("ep")
    sections = lax.axis_size("section")
    me = lax.axis_index("ep")
    sec = lax.axis_index("section")
    rows, width = states.shape
    q_cols, kv_cols, units = wq.shape[2], wk.shape[2], w_gate.shape[2]
    per_device = q_cols + 2 * kv_cols

    lengths = jnp.stack(
        [
            lax.dynamic_slice(seq_lens, (sec + 1 - tick, me * rows), (1, rows))[0]
            for tick in range(TICKS)
        ]
    )
    half = HD // 2
    inv_freq = rope_base ** (-jnp.arange(half, dtype=F32) * 2.0 / HD)
    angles = lengths.astype(F32)[:, :, None] * inv_freq[None, None, :]
    cos, sin = jnp.cos(angles), jnp.sin(angles)
    cos_t = jnp.concatenate([cos, cos], axis=-1)
    sin_t = jnp.concatenate([-sin, sin], axis=-1)

    def spread(scale):
        wide = jnp.repeat(scale[0], BLK, axis=-1)
        return wide.transpose(0, 2, 1, 3).reshape(TICKS, KVH, rows * LEN)

    place = jnp.arange(rows * LEN, dtype=jnp.int32)
    live = (place % LEN)[None, :] < jnp.repeat(lengths, LEN, axis=-1)
    same = (jnp.arange(GROUP * rows, dtype=jnp.int32) % rows)[:, None] == (place // LEN)[None, :]
    bias_t = jnp.where(same[None] & live[:, None, :], 0.0, -1e30).astype(F32)
    chosen = routes[0].transpose(0, 2, 1)
    hits_t = (chosen[..., None] == jnp.arange(EXPERTS, dtype=jnp.int32)).astype(F32)

    vmem = pl.BlockSpec(memory_space=pltpu.VMEM)
    anyspace = pl.BlockSpec(memory_space=pl.ANY)

    def buf(*shape):
        return pltpu.VMEM(shape, BF16)

    return pl.pallas_call(
        functools.partial(kernel, ep, sections),
        out_shape=jax.ShapeDtypeStruct((rows, width), BF16),
        in_specs=[vmem] * 13 + [anyspace] * 7,
        out_specs=vmem,
        scratch_shapes=[
            buf(width, q_cols),
            buf(width, kv_cols),
            buf(width, kv_cols),
            buf(q_cols, width),
            buf(width, units),
            buf(width, units),
            buf(units, width),
            buf(TICKS, rows, width),
            buf(rows, width),
            buf(rows, width),
            buf(TICKS, ep, rows, width),
            buf(TICKS, ep, rows, per_device),
            buf(TICKS, ep, rows, per_device),
            buf(TICKS, ep, rows, q_cols),
            buf(TICKS, ep, rows, q_cols),
            buf(TICKS, ep, rows, width),
            buf(TICKS, ep, rows, width),
            buf(TICKS, ep, rows, width),
            buf(ep * rows, units),
            buf(TICKS, ep, rows, width),
            buf(TICKS, ep, rows, width),
            pltpu.SemaphoreType.DMA((7,)),
            pltpu.SemaphoreType.DMA((TICKS * PHASES, ep - 1)),
            pltpu.SemaphoreType.DMA((TICKS * PHASES, ep - 1)),
            pltpu.SemaphoreType.DMA((2,)),
        ],
        compiler_params=pltpu.CompilerParams(
            collective_id=0, has_side_effects=True, vmem_limit_bytes=67043328
        ),
        name="decode_window",
    )(
        states,
        entering,
        attn_norm,
        ffn_norm,
        router,
        cache_k,
        cache_v,
        cos_t,
        sin_t,
        spread(k_scale),
        spread(v_scale),
        bias_t,
        hits_t,
        wq,
        wk,
        wv,
        wo,
        w_gate,
        w_up,
        w_down,
    )


def solution(mesh):
    return jax.shard_map(
        local,
        mesh=mesh,
        in_specs=(
            P(("section", "ep"), None),
            P("ep", None),
            P(),
            P("section", None, "ep", None),
            P("section", None),
            P("section", None),
            P("section", None, "ep"),
            P("section", None, "ep"),
            P("section", None, "ep"),
            P("section", "ep", None),
            P("section", None, None),
            P("section", None, "ep"),
            P("section", None, "ep"),
            P("section", "ep", None),
            P("section", None, "ep", None, None, None),
            P("section", None, "ep", None, None, None),
            P("section", None, "ep", None, None),
            P("section", None, "ep", None, None),
        ),
        out_specs=P(("section", "ep"), None),
        check_vma=False,
    )
```
